32 devices in a mesh: gx: 8 (over y, x, core), wa: 4 (over z).
Axes of the slice: x: 2, y: 2, z: 4, core: 2. Of those that a mesh axis runs over, the one named last changes fastest.
Arguments:
- warm_field: float32 [64, 2, 128, 2048], P('wa', None, 'gx'), may hold values from -1.8 to 1.8
- warm_adjoint: float32 [64, 2, 128, 2048], P('wa', None, 'gx'), may hold values from -1.8 to 1.8
- permittivity: float32 [128, 2048], P('gx'), may hold values from 1 to 12
- design_mask: int32 [128, 2048], P('gx'), may hold values 0 or 1
- source_row: int32 [64], P('wa'), may hold values from 0 to 127
- monitor_row: int32 [64], P('wa'), may hold values from 0 to 127
- wavenumber: float32 [64], P('wa'), may hold values from 0.02 to 0.08
- bloch_phase: float32 [64], P('wa'), may hold values from -3.140625 to 3.140625
- source_profile: float32 [64, 2, 2048], P('wa'), may hold values from -24 to 24
- monitor_profile: float32 [64, 2, 2048], P('wa'), may hold values from -4 to 4
Outputs:
- forward_field: float32 [64, 2, 128, 2048], P('wa', None, 'gx')
- adjoint_field: float32 [64, 2, 128, 2048], P('wa', None, 'gx')
- gradient: float32 [128, 2048], P('gx')
The draws below stay inside these ranges and needn't reach their ends.
All inputs are finite; a program needn't handle non-finite values. No bound on the sum of `design_mask` on one device may be relied on, other than what follows from the above.
Results may differ from the reference program's by a relative error of at most 0.0003.
Values sent between devices are 32-bit elements; how exact they have to be, the bound alone decides.
A program may use at most 128 MiB of HBM per device.

```python
import math
import jax
import jax.numpy as jnp
from jax import lax

NY = 2048
NX = 128
WAVES = 64


rough_amp = 0.01


smooth_amp = 0.3


noise_share = 0.005


def wave_kinds(key):
    ranking = jax.random.permutation(jax.random.fold_in(key, 5), WAVES)
    return ranking < max(1, WAVES // 4)


def rough_start(key):
    key_base, key_rows, key_cols = jax.random.split(key, 3)
    position = jnp.arange(NX, dtype=jnp.float32) / NX
    jitter = jax.random.uniform(key_rows, (NX,), jnp.float32, -0.15, 0.15)
    row_scale = jnp.exp(math.log(10.0) * jnp.clip(position + jitter, 0.0, 1.0))
    col_scale = jnp.exp(jax.random.uniform(key_cols, (NY,), jnp.float32, 0.0, math.log(3.0)))
    texture = jnp.clip(jax.random.normal(key_base, (WAVES, 2, NX, NY), jnp.float32), -6.0, 6.0)
    return rough_amp * texture * row_scale[:, None] * col_scale


def smooth_start(key):
    key_rotation, key_rough = jax.random.split(key)
    along_x = jnp.sin(math.pi * (jnp.arange(NX, dtype=jnp.float32) + 0.5) / NX)
    along_y = jnp.sin(math.pi * (jnp.arange(NY, dtype=jnp.float32) + 1.0) / (NY + 1))
    rotation = jax.random.uniform(key_rotation, (WAVES,), jnp.float32, -math.pi, math.pi)
    phasor = jnp.stack([jnp.cos(rotation), jnp.sin(rotation)], axis=1)
    envelope = along_x[:, None] * along_y[None, :]
    roughness = jnp.clip(jax.random.normal(key_rough, (WAVES, 2, NX, NY), jnp.float32), -6.0, 6.0)
    return smooth_amp * (phasor[:, :, None, None] * envelope + noise_share * roughness)


def blended_start(key, stream_salt):
    own_key = jax.random.fold_in(key, stream_salt)
    smooth_kind = wave_kinds(key)
    return jnp.where(smooth_kind[:, None, None, None], smooth_start(jax.random.fold_in(own_key, 1)), rough_start(jax.random.fold_in(own_key, 2)))


def profile_draw(key, stream_salt, scale, bound, weak):
    own_key = jax.random.fold_in(key, stream_salt)
    smooth_kind = wave_kinds(key)
    texture = jnp.clip(jax.random.normal(own_key, (WAVES, 2, NY), jnp.float32), -bound, bound)
    weight = jnp.where(smooth_kind, weak, 1.0)
    return scale * weight[:, None, None] * texture


def draw_warm_field(key, part):
    return blended_start(key, 11)


def draw_warm_adjoint(key, part):
    return blended_start(key, 23)


def draw_source_profile(key, part):
    return profile_draw(key, 31, 4.0, 6.0, 0.004)


def draw_monitor_profile(key, part):
    return profile_draw(key, 37, 1.0, 4.0, 0.02)


def place_ends(result, rng, least, top_value):
    shape = result.shape
    place = [jax.random.randint(jax.random.fold_in(rng, axis), (), 0, shape[axis]) for axis in range(len(shape))]
    result = result.at[tuple(place)].set(least)
    longest = shape.index(max(shape))
    place[longest] = (place[longest] + 1) % shape[longest]
    return result.at[tuple(place)].set(top_value)


def shard_levels(key, dims, shards, smallest, top_value):
    gain = 1.0
    for dim, parts in shards:
        heights = jax.random.uniform(jax.random.fold_in(jax.random.fold_in(key, 6), dim), (parts,), jnp.float32, smallest / len(shards), top_value / len(shards))
        gain = gain * jnp.repeat(jnp.exp(heights), dims[dim] // parts).reshape((-1,) + (1,) * (len(dims) - 1 - dim))
    return gain


def setup_inputs(seed: int = 0) -> dict:
    key_list = jax.random.split(jax.random.key(seed), 11)
    warm_field = draw_warm_field(jax.random.fold_in(key_list[10], 71), 0)
    warm_adjoint = draw_warm_adjoint(jax.random.fold_in(key_list[10], 71), 0)
    permittivity = jnp.clip(1.0 + 11.0 * jax.random.uniform(key_list[2], (NX, NY), jnp.float32) ** shard_levels(key_list[2], (NX, NY), ((0, 8),), -0.2, 0.2), 1.0, 12.0)
    design_mask = place_ends((jax.random.randint(key_list[3], (NX, NY), 0, 2) < 1).astype(jnp.int32), jax.random.fold_in(key_list[3], 1), 0, 1)
    source_row = place_ends(jax.random.randint(key_list[4], (WAVES,), 0, NX), jax.random.fold_in(key_list[4], 1), 0, NX - 1).astype(jnp.int32)
    monitor_row = place_ends(jax.random.randint(key_list[5], (WAVES,), 0, NX), jax.random.fold_in(key_list[5], 1), 0, NX - 1).astype(jnp.int32)
    wavenumber = jnp.clip(jnp.exp(math.log(0.08) - 1.3862944 * jax.random.uniform(key_list[6], (WAVES,), jnp.float32) ** shard_levels(key_list[6], (WAVES,), ((0, 4),), -0.2, 0.2)), 0.02, 0.08)
    bloch_phase = jnp.clip(jax.random.uniform(key_list[7], (WAVES,), jnp.float32, -3.140625, 3.140625), -3.140625, 3.140625)
    source_profile = draw_source_profile(jax.random.fold_in(key_list[10], 71), 0)
    monitor_profile = draw_monitor_profile(jax.random.fold_in(key_list[10], 71), 0)
    return dict(warm_field=warm_field, warm_adjoint=warm_adjoint, permittivity=permittivity, design_mask=design_mask, source_row=source_row, monitor_row=monitor_row, wavenumber=wavenumber, bloch_phase=bloch_phase, source_profile=source_profile, monitor_profile=monitor_profile)


floor_share = 0.5


def rotate(part, cosine, sine):
    return jnp.stack([cosine * part[0] - sine * part[1], sine * part[0] + cosine * part[1]])


def operate(field, diagonal, cosine, sine):
    above = jnp.concatenate([field[:, 1:], rotate(field[:, :1], cosine, sine)], axis=1)
    below = jnp.concatenate([rotate(field[:, -1:], cosine, -sine), field[:, :-1]], axis=1)
    zero_col = jnp.zeros_like(field[..., :1])
    y_after = jnp.concatenate([field[..., 1:], zero_col], axis=-1)
    y_before = jnp.concatenate([zero_col, field[..., :-1]], axis=-1)
    return diagonal * field - (above + below + y_after + y_before)


def complex_scale(scale_re, scale_im, vector):
    return jnp.stack([scale_re * vector[0] - scale_im * vector[1], scale_re * vector[1] + scale_im * vector[0]])


def solve_step(right_side, initial, diagonal, cosine, sine):
    residual = right_side - operate(initial, diagonal, cosine, sine)
    res_norm = jnp.sum(residual * residual)
    precond = residual / diagonal
    image = operate(precond, diagonal, cosine, sine)
    dot_re = jnp.sum(residual[0] * image[0] + residual[1] * image[1])
    dot_im = jnp.sum(residual[0] * image[1] - residual[1] * image[0])
    bounded = jnp.maximum(dot_re * dot_re + dot_im * dot_im, (floor_share * res_norm) * (floor_share * res_norm))
    step_re = res_norm * dot_re / bounded
    step_im = -res_norm * dot_im / bounded
    shrunk = residual - complex_scale(step_re, step_im, image)
    second = shrunk / diagonal
    turned = operate(second, diagonal, cosine, sine)
    ts_re = jnp.sum(turned[0] * shrunk[0] + turned[1] * shrunk[1])
    ts_im = jnp.sum(turned[0] * shrunk[1] - turned[1] * shrunk[0])
    tt_sum = jnp.sum(turned * turned)
    omega_re = ts_re / tt_sum
    omega_im = ts_im / tt_sum
    return initial + complex_scale(step_re, step_im, precond) + complex_scale(omega_re, omega_im, second)


def reference(warm_field, warm_adjoint, permittivity, design_mask, source_row, monitor_row, wavenumber, bloch_phase, source_profile, monitor_profile):
    row_index = jnp.arange(NX)

    def per_wave(running, packed):
        start_fwd, start_adj, src_at, mon_at, squared_k, phase_angle, src_prof, mon_prof = packed
        diagonal = 4.0 - squared_k * permittivity
        cosine = jnp.cos(phase_angle)
        sine = jnp.sin(phase_angle)
        src_sel = (row_index == src_at).astype(jnp.float32)[None, :, None]
        right_side = src_sel * src_prof[:, None, :]
        forward = solve_step(right_side, start_fwd, diagonal, cosine, sine)
        mon_sel = (row_index == mon_at).astype(jnp.float32)
        mon_vals = jnp.sum(mon_sel[None, :, None] * forward, axis=1)
        over_re = jnp.sum(mon_prof[0] * mon_vals[0] + mon_prof[1] * mon_vals[1])
        over_im = jnp.sum(mon_prof[0] * mon_vals[1] - mon_prof[1] * mon_vals[0])
        adj_re = over_re * mon_prof[0] - over_im * mon_prof[1]
        adj_im = -(over_re * mon_prof[1] + over_im * mon_prof[0])
        adj_side = mon_sel[None, :, None] * jnp.stack([adj_re, adj_im])[:, None, :]
        adjoint = solve_step(adj_side, start_adj, diagonal, cosine, -sine)
        contrib = 2.0 * squared_k * (adjoint[0] * forward[0] - adjoint[1] * forward[1])
        return running + contrib, (forward, adjoint)

    summed_init = jnp.zeros((NX, NY), jnp.float32)
    summed, outputs = lax.scan(per_wave, summed_init, (warm_field, warm_adjoint, source_row, monitor_row, wavenumber, bloch_phase, source_profile, monitor_profile))
    gradient = design_mask.astype(jnp.float32) * summed
    return outputs[0], outputs[1], gradient
```

```python
import functools

import jax
import jax.numpy as jnp
from jax import lax
from jax.experimental import pallas as pl
from jax.experimental.pallas import tpu as pltpu
from jax.sharding import PartitionSpec as P

floor_share = 0.5
REACH = 3
TILE = 8
SUMS = 16
VMEM_LIMIT = 48 * 1024 * 1024


def stencil(u, d, rows):
    total, width = u.shape
    col = lax.broadcasted_iota(jnp.int32, (total, width), 1)
    after = jnp.where(col == width - 1, 0.0, pltpu.roll(u, width - 1, 1))
    before = jnp.where(col == 0, 0.0, pltpu.roll(u, 1, 1))
    above = pltpu.roll(u, total - 1, 0)
    below = pltpu.roll(u, 1, 0)
    return (d * u - (above + below + after + before))[:rows]


def lay_out(ext, x_ref, hi_ref, lo_ref, scal, wave, sign):
    rows = x_ref.shape[2]
    ext[:, :rows] = x_ref[0]
    low_c, low_s, high_c, high_s = (scal[wave, i] for i in range(1, 5))
    hi_re, hi_im = hi_ref[0, 0], hi_ref[0, 1]
    lo_re, lo_im = lo_ref[0, 0], lo_ref[0, 1]
    high_s = sign * high_s
    low_s = sign * low_s
    ext[0, rows : rows + REACH] = high_c * hi_re - high_s * hi_im
    ext[1, rows : rows + REACH] = high_s * hi_re + high_c * hi_im
    ext[0, rows + TILE - REACH :] = low_c * lo_re - low_s * lo_im
    ext[1, rows + TILE - REACH :] = low_s * lo_re + low_c * lo_im


def clear_gap(ext, rows):
    @pl.when(pl.program_id(0) == 0)
    def _():
        ext[:, rows:] = jnp.zeros((2, TILE, ext.shape[2]), jnp.float32)


def residual(ext, res, d, spot, side_re, side_im):
    total = ext.shape[1]
    for part in range(2):
        res[part] = -stencil(ext[part], d, total)

    @pl.when(spot >= 0)
    def _():
        res[0, pl.ds(spot, 1)] = res[0, pl.ds(spot, 1)] + side_re
        res[1, pl.ds(spot, 1)] = res[1, pl.ds(spot, 1)] + side_im


def fold(cells):
    width = cells.shape[1]
    acc = cells[:, :128]
    for start in range(128, width, 128):
        acc = acc + cells[:, start : start + 128]
    return jnp.sum(acc, axis=0, keepdims=True)


def put_dots(out, r, v, w):
    out[0, 0:1] = fold(r[0] * r[0] + r[1] * r[1])
    out[0, 1:2] = fold(r[0] * v[0] + r[1] * v[1])
    out[0, 2:3] = fold(r[0] * v[1] - r[1] * v[0])
    out[0, 3:4] = fold(v[0] * v[0] + v[1] * v[1])
    out[0, 4:5] = fold(w[0] * r[0] + w[1] * r[1])
    out[0, 5:6] = fold(w[0] * r[1] - w[1] * r[0])
    out[0, 6:7] = fold(w[0] * v[0] + w[1] * v[1])
    out[0, 7:8] = fold(w[0] * v[1] - w[1] * v[0])
    out[0, 8:9] = fold(w[0] * w[0] + w[1] * w[1])


def images(res, d, inv, rows, deep, keep=None):
    total = res.shape[1]
    z = [res[part] * inv for part in range(2)]
    v = [stencil(z[part], d, total if deep else rows) for part in range(2)]
    if not deep:
        return [u[:rows] for u in z], v, None
    y = [v[part] * inv for part in range(2)]
    if keep is not None:
        keep(z, y)
    w = [stencil(y[part], d, rows) for part in range(2)]
    return z, [u[:rows] for u in v], w


def side_row(profile_re, profile_im, scal, wave, slot):
    turn_c, turn_s = scal[wave, slot], scal[wave, slot + 1]
    return (
        turn_c * profile_re - turn_s * profile_im,
        turn_s * profile_re + turn_c * profile_im,
    )


def first_pass(
    scal, spots, eps, x_ref, hi_ref, lo_ref, src_ref, mon_ref, out, ext, res, zed, yed
):
    wave = pl.program_id(0)
    rows = x_ref.shape[2]
    clear_gap(ext, rows)
    lay_out(ext, x_ref, hi_ref, lo_ref, scal, wave, 1.0)
    d = 4.0 - scal[wave, 0] * eps[...]
    inv = 1.0 / d
    side_re, side_im = side_row(src_ref[0, 0:1], src_ref[0, 1:2], scal, wave, 5)
    residual(ext, res, d, spots[wave, 0], side_re, side_im)

    def keep(z, y):
        for part in range(2):
            zed[part] = z[part][:rows]
            yed[part] = y[part][:rows]

    z, v, w = images(res, d, inv, rows, True, keep)
    r = [res[part, :rows] for part in range(2)]
    put_dots(out, r, v, w)
    out[0, 9:SUMS] = jnp.zeros((SUMS - 9, 128), jnp.float32)
    mon = spots[wave, 1]

    @pl.when((mon >= 0) & (mon < rows))
    def _():
        m_re, m_im = mon_ref[0, 0:1], mon_ref[0, 1:2]
        for slot, held in ((9, ext), (11, zed), (13, yed)):
            f_re, f_im = held[0, pl.ds(mon, 1)], held[1, pl.ds(mon, 1)]
            out[0, slot : slot + 1] = fold(m_re * f_re + m_im * f_im)
            out[0, slot + 1 : slot + 2] = fold(m_re * f_im - m_im * f_re)


def step_result(ext, res, z, v, inv, coef, wave, rows):
    a_re, a_im, o_re, o_im = (coef[wave, i] for i in range(4))
    x = [ext[part, :rows] for part in range(2)]
    r = [res[part, :rows] for part in range(2)]
    inv = inv[:rows]
    y_re = (r[0] - (a_re * v[0] - a_im * v[1])) * inv
    y_im = (r[1] - (a_re * v[1] + a_im * v[0])) * inv
    out_re = x[0] + (a_re * z[0] - a_im * z[1]) + (o_re * y_re - o_im * y_im)
    out_im = x[1] + (a_re * z[1] + a_im * z[0]) + (o_re * y_im + o_im * y_re)
    return out_re, out_im


def adjoint_row(mon_ref, coef, scal, wave):
    over_re, over_im = coef[wave, 4], coef[wave, 5]
    m_re, m_im = mon_ref[0, 0:1], mon_ref[0, 1:2]
    adj_re = over_re * m_re - over_im * m_im
    adj_im = -(over_re * m_im + over_im * m_re)
    return side_row(adj_re, adj_im, scal, wave, 7)


def second_pass(
    scal, spots, coef, eps, x_ref, hi_ref, lo_ref, ax_ref, ahi_ref, alo_ref, src_ref, mon_ref,
    fwd, out, ext, res, aext, ares,
):
    wave = pl.program_id(0)
    rows = x_ref.shape[2]
    clear_gap(ext, rows)
    clear_gap(aext, rows)
    d = 4.0 - scal[wave, 0] * eps[...]
    inv = 1.0 / d
    lay_out(ext, x_ref, hi_ref, lo_ref, scal, wave, 1.0)
    side_re, side_im = side_row(src_ref[0, 0:1], src_ref[0, 1:2], scal, wave, 5)
    residual(ext, res, d, spots[wave, 0], side_re, side_im)
    z, v, _ = images(res, d, inv, rows, False)
    fwd[0, 0], fwd[0, 1] = step_result(ext, res, z, v, inv, coef, wave, rows)

    lay_out(aext, ax_ref, ahi_ref, alo_ref, scal, wave, -1.0)
    adj_re, adj_im = adjoint_row(mon_ref, coef, scal, wave)
    residual(aext, ares, d, spots[wave, 1], adj_re, adj_im)
    z, v, w = images(ares, d, inv, rows, True)
    put_dots(out, [ares[part, :rows] for part in range(2)], v, w)
    out[0, 9:SUMS] = jnp.zeros((SUMS - 9, 128), jnp.float32)


def third_pass(
    scal, spots, coef, acoef, eps, ax_ref, ahi_ref, alo_ref, mon_ref, fwd, adj, grad, aext, ares
):
    wave = pl.program_id(0)
    rows = ax_ref.shape[2]
    clear_gap(aext, rows)
    d = 4.0 - scal[wave, 0] * eps[...]
    inv = 1.0 / d
    lay_out(aext, ax_ref, ahi_ref, alo_ref, scal, wave, -1.0)
    adj_re, adj_im = adjoint_row(mon_ref, coef, scal, wave)
    residual(aext, ares, d, spots[wave, 1], adj_re, adj_im)
    z, v, _ = images(ares, d, inv, rows, False)
    out_re, out_im = step_result(aext, ares, z, v, inv, acoef, wave, rows)
    adj[0, 0] = out_re
    adj[0, 1] = out_im
    term = (2.0 * scal[wave, 0]) * (out_re * fwd[0, 0] - out_im * fwd[0, 1])

    @pl.when(wave == 0)
    def _():
        grad[...] = term

    @pl.when(wave > 0)
    def _():
        grad[...] = grad[...] + term


def greet(axis, count, me):
    barrier = pltpu.get_barrier_semaphore()
    for hop in range(1, count):
        pl.semaphore_signal(
            barrier, inc=1, device_id={axis: lax.rem(me + hop, count)},
            device_id_type=pl.DeviceIdType.MESH,
        )
    pl.semaphore_wait(barrier, count - 1)


def sum_kernel(count, with_overlap, parts, coef, mine, got, send_sem, recv_sem):
    me = lax.axis_index("gx")
    local_sum = jnp.sum(parts[...], axis=-1)
    mine[...] = local_sum
    greet("gx", count, me)

    def move(hop, place):
        return pltpu.make_async_remote_copy(
            src_ref=mine, dst_ref=got.at[place], send_sem=send_sem.at[hop],
            recv_sem=recv_sem.at[hop], device_id={"gx": lax.rem(me + hop, count)},
            device_id_type=pl.DeviceIdType.MESH,
        )

    for hop in range(1, count):
        move(hop, me).start()
    got[me] = local_sum
    for hop in range(1, count):
        move(hop, lax.rem(me - hop + count, count)).wait_recv()
    total = got[0]
    for place in range(1, count):
        total = total + got[place]
    q = [total[:, i : i + 1] for i in range(SUMS)]
    res_norm, rv_re, rv_im, image_sq, wr_re, wr_im, wv_re, wv_im, twice_sq = q[:9]
    half = floor_share * res_norm
    bounded = jnp.maximum(rv_re * rv_re + rv_im * rv_im, half * half)
    step_re = res_norm * rv_re / bounded
    step_im = -res_norm * rv_im / bounded
    step_sq = step_re * step_re + step_im * step_im
    ts_re = rv_re - step_re * image_sq - (step_re * wr_re + step_im * wr_im) + step_sq * wv_re
    ts_im = -rv_im - step_im * image_sq - (step_re * wr_im - step_im * wr_re) + step_sq * wv_im
    tt_sum = image_sq - 2.0 * (step_re * wv_re + step_im * wv_im) + step_sq * twice_sq
    omega_re = ts_re / tt_sum
    omega_im = ts_im / tt_sum
    found = [step_re, step_im, omega_re, omega_im]
    if with_overlap:
        mx_re, mx_im, mz_re, mz_im, my_re, my_im = q[9:15]
        ms_re = mz_re - (step_re * my_re - step_im * my_im)
        ms_im = mz_im - (step_re * my_im + step_im * my_re)
        found.append(
            mx_re + (step_re * mz_re - step_im * mz_im) + (omega_re * ms_re - omega_im * ms_im)
        )
        found.append(
            mx_im + (step_re * mz_im + step_im * mz_re) + (omega_re * ms_im + omega_im * ms_re)
        )
    lane = lax.broadcasted_iota(jnp.int32, coef.shape, 1)
    packed = jnp.zeros(coef.shape, jnp.float32)
    for i, value in enumerate(found):
        packed = jnp.where(lane == i, value, packed)
    coef[...] = packed
    for hop in range(1, count):
        move(hop, me).wait_send()


def sum_over_gx(parts, with_overlap, ident):
    count = lax.axis_size("gx")
    waves = parts.shape[0]
    return pl.pallas_call(
        functools.partial(sum_kernel, count, with_overlap),
        out_shape=jax.ShapeDtypeStruct((waves, SUMS), jnp.float32),
        in_specs=[pl.BlockSpec(memory_space=pltpu.VMEM)],
        out_specs=pl.BlockSpec(memory_space=pltpu.VMEM),
        scratch_shapes=[
            pltpu.VMEM((waves, SUMS), jnp.float32),
            pltpu.VMEM((count, waves, SUMS), jnp.float32),
            pltpu.SemaphoreType.DMA((count,)),
            pltpu.SemaphoreType.DMA((count,)),
        ],
        compiler_params=pltpu.CompilerParams(collective_id=ident, has_side_effects=True),
        name="sum_first" if with_overlap else "sum_second",
    )(parts)


def gradient_kernel(count, part_ref, mask_ref, out, got, total, spread, sems):
    me = lax.axis_index("wa")
    width = part_ref.shape[1] // count

    def columns(place):
        return pl.ds(pl.multiple_of(place * width, 128), width)

    greet("wa", count, me)

    def scatter(hop, place):
        to = lax.rem(me + hop, count)
        return pltpu.make_async_remote_copy(
            src_ref=part_ref.at[:, columns(to)], dst_ref=got.at[place],
            send_sem=sems.at[0, hop], recv_sem=sems.at[1, hop],
            device_id={"wa": to}, device_id_type=pl.DeviceIdType.MESH,
        )

    def gather(hop, place):
        return pltpu.make_async_remote_copy(
            src_ref=total, dst_ref=spread.at[place],
            send_sem=sems.at[2, hop], recv_sem=sems.at[3, hop],
            device_id={"wa": lax.rem(me + hop, count)}, device_id_type=pl.DeviceIdType.MESH,
        )

    for hop in range(1, count):
        scatter(hop, me).start()
    got[me] = part_ref[:, columns(me)]
    for hop in range(1, count):
        scatter(hop, lax.rem(me - hop + count, count)).wait_recv()
    summed = got[0]
    for place in range(1, count):
        summed = summed + got[place]
    total[...] = summed
    for hop in range(1, count):
        gather(hop, me).start()
    spread[me] = summed
    for hop in range(1, count):
        gather(hop, lax.rem(me - hop + count, count)).wait_recv()
    for place in range(count):
        span = slice(place * width, (place + 1) * width)
        out[:, span] = mask_ref[:, span].astype(jnp.float32) * spread[place]
    for hop in range(1, count):
        scatter(hop, me).wait_send()
        gather(hop, me).wait_send()


def gradient_sum(part, mask):
    count = lax.axis_size("wa")
    rows, width = part.shape
    piece = (rows, width // count)
    return pl.pallas_call(
        functools.partial(gradient_kernel, count),
        out_shape=jax.ShapeDtypeStruct(part.shape, jnp.float32),
        in_specs=[pl.BlockSpec(memory_space=pltpu.VMEM)] * 2,
        out_specs=pl.BlockSpec(memory_space=pltpu.VMEM),
        scratch_shapes=[
            pltpu.VMEM((count, *piece), jnp.float32),
            pltpu.VMEM(piece, jnp.float32),
            pltpu.VMEM((count, *piece), jnp.float32),
            pltpu.SemaphoreType.DMA((4, count)),
        ],
        compiler_params=pltpu.CompilerParams(collective_id=2, has_side_effects=True),
        name="sum_gradient",
    )(part, mask)


def neighbours(cells, dim, reach):
    count = lax.axis_size("gx")
    extent = cells.shape[dim]
    head = lax.slice_in_dim(cells, 0, reach, axis=dim)
    tail = lax.slice_in_dim(cells, extent - reach, extent, axis=dim)
    hi = lax.ppermute(head, "gx", [((i + 1) % count, i) for i in range(count)])
    lo = lax.ppermute(tail, "gx", [(i, (i + 1) % count) for i in range(count)])
    return hi, lo


def local(
    warm_field,
    warm_adjoint,
    permittivity,
    design_mask,
    source_row,
    monitor_row,
    wavenumber,
    bloch_phase,
    source_profile,
    monitor_profile,
):
    waves, _, rows, width = warm_field.shape
    total = rows + TILE
    count = lax.axis_size("gx")
    whole = rows * count
    me = lax.axis_index("gx")
    at_first, at_last = me == 0, me == count - 1
    cosine, sine = jnp.cos(bloch_phase), jnp.sin(bloch_phase)
    one, zero = jnp.ones_like(cosine), jnp.zeros_like(cosine)
    low_c = jnp.where(at_first, cosine, one)
    low_s = jnp.where(at_first, -sine, zero)
    high_c = jnp.where(at_last, cosine, one)
    high_s = jnp.where(at_last, sine, zero)

    def spot_of(row):
        away = jnp.remainder(row - me * rows, whole)
        spot = jnp.where(
            away < rows + REACH, away,
            jnp.where(away >= whole - REACH, away - whole + total, -1),
        )
        above = (spot >= rows) & (spot < rows + REACH)
        below = spot >= rows + REACH
        turn_c = jnp.where(above, high_c, jnp.where(below, low_c, one))
        turn_s = jnp.where(above, high_s, jnp.where(below, low_s, zero))
        return spot, turn_c, turn_s

    src_spot, src_c, src_s = spot_of(source_row)
    mon_spot, mon_c, mon_s = spot_of(monitor_row)
    scal = jnp.stack(
        [wavenumber, low_c, low_s, high_c, high_s, src_c, src_s, mon_c, -mon_s], axis=1
    )
    spots = jnp.stack([src_spot, mon_spot], axis=1)
    eps_hi, eps_lo = neighbours(permittivity, 0, REACH)
    eps = jnp.concatenate(
        [permittivity, eps_hi, jnp.ones((TILE - 2 * REACH, width), jnp.float32), eps_lo], axis=0
    )
    hi, lo = neighbours(warm_field, 2, REACH)
    ahi, alo = neighbours(warm_adjoint, 2, REACH)

    smem = pl.BlockSpec(memory_space=pltpu.SMEM)
    field_spec = pl.BlockSpec((1, 2, rows, width), lambda w: (w, 0, 0, 0))
    rim_spec = pl.BlockSpec((1, 2, REACH, width), lambda w: (w, 0, 0, 0))
    row_spec = pl.BlockSpec((1, 2, width), lambda w: (w, 0, 0))
    eps_spec = pl.BlockSpec((total, width), lambda w: (0, 0))
    dot_spec = pl.BlockSpec((1, SUMS, 128), lambda w: (w, 0, 0))
    grad_spec = pl.BlockSpec((rows, width), lambda w: (0, 0))
    field_shape = jax.ShapeDtypeStruct(warm_field.shape, jnp.float32)
    dot_shape = jax.ShapeDtypeStruct((waves, SUMS, 128), jnp.float32)
    ext_shape = pltpu.VMEM((2, total, width), jnp.float32)
    flat_shape = pltpu.VMEM((2, rows, width), jnp.float32)
    params = pltpu.CompilerParams(
        dimension_semantics=("arbitrary",), vmem_limit_bytes=VMEM_LIMIT
    )
    field_bytes = 4 * waves * 2 * rows * width

    def cost(ops, fields):
        return pl.CostEstimate(
            flops=ops * field_bytes // 4, bytes_accessed=fields * field_bytes, transcendentals=0
        )

    dots = pl.pallas_call(
        first_pass,
        grid=(waves,),
        out_shape=dot_shape,
        in_specs=[smem, smem, eps_spec, field_spec, rim_spec, rim_spec, row_spec, row_spec],
        out_specs=dot_spec,
        scratch_shapes=[ext_shape, ext_shape, flat_shape, flat_shape],
        compiler_params=params,
        cost_estimate=cost(60, 1),
        name="first_pass",
    )(scal, spots, eps, warm_field, hi, lo, source_profile, monitor_profile)
    coef = sum_over_gx(dots, True, 0)
    forward, adots = pl.pallas_call(
        second_pass,
        grid=(waves,),
        out_shape=(field_shape, dot_shape),
        in_specs=[smem, smem, smem, eps_spec]
        + [field_spec, rim_spec, rim_spec] * 2
        + [row_spec, row_spec],
        out_specs=(field_spec, dot_spec),
        scratch_shapes=[ext_shape] * 4,
        compiler_params=params,
        cost_estimate=cost(100, 3),
        name="second_pass",
    )(
        scal, spots, coef, eps, warm_field, hi, lo, warm_adjoint, ahi, alo,
        source_profile, monitor_profile,
    )
    acoef = sum_over_gx(adots, False, 1)
    adjoint, grad_part = pl.pallas_call(
        third_pass,
        grid=(waves,),
        out_shape=(field_shape, jax.ShapeDtypeStruct((rows, width), jnp.float32)),
        in_specs=[smem, smem, smem, smem, eps_spec, field_spec, rim_spec, rim_spec, row_spec,
                  field_spec],
        out_specs=(field_spec, grad_spec),
        scratch_shapes=[ext_shape] * 2,
        compiler_params=params,
        cost_estimate=cost(50, 3),
        name="third_pass",
    )(scal, spots, coef, acoef, eps, warm_adjoint, ahi, alo, monitor_profile, forward)
    gradient = gradient_sum(grad_part, design_mask)
    return (forward, adjoint, gradient)


def solution(mesh):
    placed = (
        P("wa", None, "gx", None),
        P("wa", None, "gx", None),
        P("gx", None),
        P("gx", None),
        P("wa"),
        P("wa"),
        P("wa"),
        P("wa"),
        P("wa", None, None),
        P("wa", None, None),
    )
    return jax.shard_map(
        local,
        mesh=mesh,
        in_specs=placed,
        out_specs=(P("wa", None, "gx", None), P("wa", None, "gx", None), P("gx", None)),
        check_vma=False,
    )
```

```python
import functools

import jax
import jax.numpy as jnp
from jax import lax
from jax.experimental import pallas as pl
from jax.experimental.pallas import tpu as pltpu
from jax.sharding import PartitionSpec as P

floor_share = 0.5
REACH = 3
TILE = 8
SUMS = 16
VMEM_LIMIT = 60 * 1024 * 1024


def edge_free(u, step):
    width = u.shape[1]
    turned = pltpu.roll(u, step % width, 1)
    lane = lax.broadcasted_iota(jnp.int32, (u.shape[0], 128), 1)
    if step < 0:
        end = jnp.where(lane == 127, 0.0, turned[:, width - 128 :])
        return jnp.concatenate([turned[:, : width - 128], end], axis=1)
    end = jnp.where(lane == 0, 0.0, turned[:, :128])
    return jnp.concatenate([end, turned[:, 128:]], axis=1)


def stencil(u, d, rows):
    total = u.shape[0]
    above = pltpu.roll(u, total - 1, 0)[:rows]
    below = pltpu.roll(u, 1, 0)[:rows]
    u = u[:rows]
    return d[:rows] * u - (above + below + edge_free(u, -1) + edge_free(u, 1))


def lay_out(ext, x_ref, hi_ref, lo_ref, scal, wave, sign):
    rows = x_ref.shape[2]
    ext[:, :rows] = x_ref[0]
    low_c, low_s, high_c, high_s = (scal[wave, i] for i in range(1, 5))
    hi_re, hi_im = hi_ref[0, 0], hi_ref[0, 1]
    lo_re, lo_im = lo_ref[0, 0], lo_ref[0, 1]
    high_s = sign * high_s
    low_s = sign * low_s
    ext[0, rows : rows + REACH] = high_c * hi_re - high_s * hi_im
    ext[1, rows : rows + REACH] = high_s * hi_re + high_c * hi_im
    ext[0, rows + TILE - REACH :] = low_c * lo_re - low_s * lo_im
    ext[1, rows + TILE - REACH :] = low_s * lo_re + low_c * lo_im


def clear_gap(ext, rows):
    @pl.when(pl.program_id(0) == 0)
    def _():
        ext[:, rows:] = jnp.zeros((2, TILE, ext.shape[2]), jnp.float32)


def residual(ext, res, d, spot, side_re, side_im):
    total = ext.shape[1]
    for part in range(2):
        res[part] = -stencil(ext[part], d, total)

    @pl.when(spot >= 0)
    def _():
        res[0, pl.ds(spot, 1)] = res[0, pl.ds(spot, 1)] + side_re
        res[1, pl.ds(spot, 1)] = res[1, pl.ds(spot, 1)] + side_im


def fold(cells):
    width = cells.shape[1]
    acc = cells[:, :128]
    for start in range(128, width, 128):
        acc = acc + cells[:, start : start + 128]
    return jnp.sum(acc, axis=0, keepdims=True)


def put_dots(out, r, v, w):
    out[0, 0:1] = fold(r[0] * r[0] + r[1] * r[1])
    out[0, 1:2] = fold(r[0] * v[0] + r[1] * v[1])
    out[0, 2:3] = fold(r[0] * v[1] - r[1] * v[0])
    out[0, 3:4] = fold(v[0] * v[0] + v[1] * v[1])
    out[0, 4:5] = fold(w[0] * r[0] + w[1] * r[1])
    out[0, 5:6] = fold(w[0] * r[1] - w[1] * r[0])
    out[0, 6:7] = fold(w[0] * v[0] + w[1] * v[1])
    out[0, 7:8] = fold(w[0] * v[1] - w[1] * v[0])
    out[0, 8:9] = fold(w[0] * w[0] + w[1] * w[1])


def images(res, d, inv, rows, deep, keep=None):
    total = res.shape[1]
    z = [res[part] * inv for part in range(2)]
    v = [stencil(z[part], d, total if deep else rows) for part in range(2)]
    if not deep:
        return [u[:rows] for u in z], v, None
    y = [v[part] * inv for part in range(2)]
    if keep is not None:
        keep(z, y)
    w = [stencil(y[part], d, rows) for part in range(2)]
    return z, [u[:rows] for u in v], w


def side_row(profile_re, profile_im, scal, wave, slot):
    turn_c, turn_s = scal[wave, slot], scal[wave, slot + 1]
    return (
        turn_c * profile_re - turn_s * profile_im,
        turn_s * profile_re + turn_c * profile_im,
    )


def first_pass(
    scal, spots, eps, x_ref, hi_ref, lo_ref, src_ref, mon_ref, out, ext, res, zed, yed
):
    wave = pl.program_id(0)
    rows = x_ref.shape[2]
    clear_gap(ext, rows)
    lay_out(ext, x_ref, hi_ref, lo_ref, scal, wave, 1.0)
    d = 4.0 - scal[wave, 0] * eps[...]
    inv = 1.0 / d
    side_re, side_im = side_row(src_ref[0, 0:1], src_ref[0, 1:2], scal, wave, 5)
    residual(ext, res, d, spots[wave, 0], side_re, side_im)

    def keep(z, y):
        for part in range(2):
            zed[part] = z[part][:rows]
            yed[part] = y[part][:rows]

    z, v, w = images(res, d, inv, rows, True, keep)
    r = [res[part, :rows] for part in range(2)]
    put_dots(out, r, v, w)
    out[0, 9:SUMS] = jnp.zeros((SUMS - 9, 128), jnp.float32)
    mon = spots[wave, 1]

    @pl.when((mon >= 0) & (mon < rows))
    def _():
        m_re, m_im = mon_ref[0, 0:1], mon_ref[0, 1:2]
        for slot, held in ((9, ext), (11, zed), (13, yed)):
            f_re, f_im = held[0, pl.ds(mon, 1)], held[1, pl.ds(mon, 1)]
            out[0, slot : slot + 1] = fold(m_re * f_re + m_im * f_im)
            out[0, slot + 1 : slot + 2] = fold(m_re * f_im - m_im * f_re)


def step_result(ext, res, z, v, inv, coef, wave, rows):
    a_re, a_im, o_re, o_im = (coef[wave, i] for i in range(4))
    x = [ext[part, :rows] for part in range(2)]
    r = [res[part, :rows] for part in range(2)]
    inv = inv[:rows]
    y_re = (r[0] - (a_re * v[0] - a_im * v[1])) * inv
    y_im = (r[1] - (a_re * v[1] + a_im * v[0])) * inv
    out_re = x[0] + (a_re * z[0] - a_im * z[1]) + (o_re * y_re - o_im * y_im)
    out_im = x[1] + (a_re * z[1] + a_im * z[0]) + (o_re * y_im + o_im * y_re)
    return out_re, out_im


def adjoint_row(mon_ref, coef, scal, wave):
    over_re, over_im = coef[wave, 4], coef[wave, 5]
    m_re, m_im = mon_ref[0, 0:1], mon_ref[0, 1:2]
    adj_re = over_re * m_re - over_im * m_im
    adj_im = -(over_re * m_im + over_im * m_re)
    return side_row(adj_re, adj_im, scal, wave, 7)


def second_pass(
    scal, spots, coef, eps, x_ref, hi_ref, lo_ref, ax_ref, ahi_ref, alo_ref, src_ref, mon_ref,
    fwd, out, ext, res, aext, ares,
):
    wave = pl.program_id(0)
    rows = x_ref.shape[2]
    clear_gap(ext, rows)
    clear_gap(aext, rows)
    d = 4.0 - scal[wave, 0] * eps[...]
    inv = 1.0 / d
    lay_out(ext, x_ref, hi_ref, lo_ref, scal, wave, 1.0)
    side_re, side_im = side_row(src_ref[0, 0:1], src_ref[0, 1:2], scal, wave, 5)
    residual(ext, res, d, spots[wave, 0], side_re, side_im)
    z, v, _ = images(res, d, inv, rows, False)
    fwd[0, 0], fwd[0, 1] = step_result(ext, res, z, v, inv, coef, wave, rows)

    lay_out(aext, ax_ref, ahi_ref, alo_ref, scal, wave, -1.0)
    adj_re, adj_im = adjoint_row(mon_ref, coef, scal, wave)
    residual(aext, ares, d, spots[wave, 1], adj_re, adj_im)
    z, v, w = images(ares, d, inv, rows, True)
    put_dots(out, [ares[part, :rows] for part in range(2)], v, w)
    out[0, 9:SUMS] = jnp.zeros((SUMS - 9, 128), jnp.float32)


def third_pass(
    scal, spots, coef, acoef, eps, ax_ref, ahi_ref, alo_ref, mon_ref, fwd, adj, grad, aext, ares
):
    wave = pl.program_id(0)
    rows = ax_ref.shape[2]
    clear_gap(aext, rows)
    d = 4.0 - scal[wave, 0] * eps[...]
    inv = 1.0 / d
    lay_out(aext, ax_ref, ahi_ref, alo_ref, scal, wave, -1.0)
    adj_re, adj_im = adjoint_row(mon_ref, coef, scal, wave)
    residual(aext, ares, d, spots[wave, 1], adj_re, adj_im)
    z, v, _ = images(ares, d, inv, rows, False)
    out_re, out_im = step_result(aext, ares, z, v, inv, acoef, wave, rows)
    adj[0, 0] = out_re
    adj[0, 1] = out_im
    term = (2.0 * scal[wave, 0]) * (out_re * fwd[0, 0] - out_im * fwd[0, 1])

    @pl.when(wave == 0)
    def _():
        grad[...] = term

    @pl.when(wave > 0)
    def _():
        grad[...] = grad[...] + term


def greet(axis, count, me):
    barrier = pltpu.get_barrier_semaphore()
    for hop in range(1, count):
        pl.semaphore_signal(
            barrier, inc=1, device_id={axis: lax.rem(me + hop, count)},
            device_id_type=pl.DeviceIdType.MESH,
        )
    pl.semaphore_wait(barrier, count - 1)


def sum_kernel(count, with_overlap, parts, coef, mine, got, send_sem, recv_sem):
    me = lax.axis_index("gx")
    local_sum = jnp.sum(parts[...], axis=-1)
    mine[...] = local_sum
    greet("gx", count, me)

    def move(hop, place):
        return pltpu.make_async_remote_copy(
            src_ref=mine, dst_ref=got.at[place], send_sem=send_sem.at[hop],
            recv_sem=recv_sem.at[hop], device_id={"gx": lax.rem(me + hop, count)},
            device_id_type=pl.DeviceIdType.MESH,
        )

    for hop in range(1, count):
        move(hop, me).start()
    got[me] = local_sum
    for hop in range(1, count):
        move(hop, lax.rem(me - hop + count, count)).wait_recv()
    total = got[0]
    for place in range(1, count):
        total = total + got[place]
    q = [total[:, i : i + 1] for i in range(SUMS)]
    res_norm, rv_re, rv_im, image_sq, wr_re, wr_im, wv_re, wv_im, twice_sq = q[:9]
    half = floor_share * res_norm
    bounded = jnp.maximum(rv_re * rv_re + rv_im * rv_im, half * half)
    step_re = res_norm * rv_re / bounded
    step_im = -res_norm * rv_im / bounded
    step_sq = step_re * step_re + step_im * step_im
    ts_re = rv_re - step_re * image_sq - (step_re * wr_re + step_im * wr_im) + step_sq * wv_re
    ts_im = -rv_im - step_im * image_sq - (step_re * wr_im - step_im * wr_re) + step_sq * wv_im
    tt_sum = image_sq - 2.0 * (step_re * wv_re + step_im * wv_im) + step_sq * twice_sq
    omega_re = ts_re / tt_sum
    omega_im = ts_im / tt_sum
    found = [step_re, step_im, omega_re, omega_im]
    if with_overlap:
        mx_re, mx_im, mz_re, mz_im, my_re, my_im = q[9:15]
        ms_re = mz_re - (step_re * my_re - step_im * my_im)
        ms_im = mz_im - (step_re * my_im + step_im * my_re)
        found.append(
            mx_re + (step_re * mz_re - step_im * mz_im) + (omega_re * ms_re - omega_im * ms_im)
        )
        found.append(
            mx_im + (step_re * mz_im + step_im * mz_re) + (omega_re * ms_im + omega_im * ms_re)
        )
    lane = lax.broadcasted_iota(jnp.int32, coef.shape, 1)
    packed = jnp.zeros(coef.shape, jnp.float32)
    for i, value in enumerate(found):
        packed = jnp.where(lane == i, value, packed)
    coef[...] = packed
    for hop in range(1, count):
        move(hop, me).wait_send()


def sum_over_gx(parts, with_overlap, ident):
    count = lax.axis_size("gx")
    waves = parts.shape[0]
    return pl.pallas_call(
        functools.partial(sum_kernel, count, with_overlap),
        out_shape=jax.ShapeDtypeStruct((waves, SUMS), jnp.float32),
        in_specs=[pl.BlockSpec(memory_space=pltpu.VMEM)],
        out_specs=pl.BlockSpec(memory_space=pltpu.VMEM),
        scratch_shapes=[
            pltpu.VMEM((waves, SUMS), jnp.float32),
            pltpu.VMEM((count, waves, SUMS), jnp.float32),
            pltpu.SemaphoreType.DMA((count,)),
            pltpu.SemaphoreType.DMA((count,)),
        ],
        compiler_params=pltpu.CompilerParams(collective_id=ident, has_side_effects=True),
        name="sum_first" if with_overlap else "sum_second",
    )(parts)


def gradient_kernel(count, part_ref, mask_ref, out, got, total, spread, sems):
    me = lax.axis_index("wa")
    width = part_ref.shape[1] // count

    def columns(place):
        return pl.ds(pl.multiple_of(place * width, 128), width)

    greet("wa", count, me)

    def scatter(hop, place):
        to = lax.rem(me + hop, count)
        return pltpu.make_async_remote_copy(
            src_ref=part_ref.at[:, columns(to)], dst_ref=got.at[place],
            send_sem=sems.at[0, hop], recv_sem=sems.at[1, hop],
            device_id={"wa": to}, device_id_type=pl.DeviceIdType.MESH,
        )

    def gather(hop, place):
        return pltpu.make_async_remote_copy(
            src_ref=total, dst_ref=spread.at[place],
            send_sem=sems.at[2, hop], recv_sem=sems.at[3, hop],
            device_id={"wa": lax.rem(me + hop, count)}, device_id_type=pl.DeviceIdType.MESH,
        )

    for hop in range(1, count):
        scatter(hop, me).start()
    got[me] = part_ref[:, columns(me)]
    for hop in range(1, count):
        scatter(hop, lax.rem(me - hop + count, count)).wait_recv()
    summed = got[0]
    for place in range(1, count):
        summed = summed + got[place]
    total[...] = summed
    for hop in range(1, count):
        gather(hop, me).start()
    spread[me] = summed
    for hop in range(1, count):
        gather(hop, lax.rem(me - hop + count, count)).wait_recv()
    for place in range(count):
        span = slice(place * width, (place + 1) * width)
        out[:, span] = mask_ref[:, span].astype(jnp.float32) * spread[place]
    for hop in range(1, count):
        scatter(hop, me).wait_send()
        gather(hop, me).wait_send()


def gradient_sum(part, mask):
    count = lax.axis_size("wa")
    rows, width = part.shape
    piece = (rows, width // count)
    return pl.pallas_call(
        functools.partial(gradient_kernel, count),
        out_shape=jax.ShapeDtypeStruct(part.shape, jnp.float32),
        in_specs=[pl.BlockSpec(memory_space=pltpu.VMEM)] * 2,
        out_specs=pl.BlockSpec(memory_space=pltpu.VMEM),
        scratch_shapes=[
            pltpu.VMEM((count, *piece), jnp.float32),
            pltpu.VMEM(piece, jnp.float32),
            pltpu.VMEM((count, *piece), jnp.float32),
            pltpu.SemaphoreType.DMA((4, count)),
        ],
        compiler_params=pltpu.CompilerParams(collective_id=2, has_side_effects=True),
        name="sum_gradient",
    )(part, mask)


def ends(cells, dim, reach):
    extent = cells.shape[dim]
    head = lax.slice_in_dim(cells, 0, reach, axis=dim)
    tail = lax.slice_in_dim(cells, extent - reach, extent, axis=dim)
    return head, tail


def neighbours(head, tail):
    count = lax.axis_size("gx")
    hi = lax.ppermute(head, "gx", [((i + 1) % count, i) for i in range(count)])
    lo = lax.ppermute(tail, "gx", [(i, (i + 1) % count) for i in range(count)])
    return hi, lo


def local(
    warm_field,
    warm_adjoint,
    permittivity,
    design_mask,
    source_row,
    monitor_row,
    wavenumber,
    bloch_phase,
    source_profile,
    monitor_profile,
):
    waves, _, rows, width = warm_field.shape
    total = rows + TILE
    count = lax.axis_size("gx")
    whole = rows * count
    me = lax.axis_index("gx")
    at_first, at_last = me == 0, me == count - 1
    cosine, sine = jnp.cos(bloch_phase), jnp.sin(bloch_phase)
    one, zero = jnp.ones_like(cosine), jnp.zeros_like(cosine)
    low_c = jnp.where(at_first, cosine, one)
    low_s = jnp.where(at_first, -sine, zero)
    high_c = jnp.where(at_last, cosine, one)
    high_s = jnp.where(at_last, sine, zero)

    def spot_of(row):
        away = jnp.remainder(row - me * rows, whole)
        spot = jnp.where(
            away < rows + REACH, away,
            jnp.where(away >= whole - REACH, away - whole + total, -1),
        )
        above = (spot >= rows) & (spot < rows + REACH)
        below = spot >= rows + REACH
        turn_c = jnp.where(above, high_c, jnp.where(below, low_c, one))
        turn_s = jnp.where(above, high_s, jnp.where(below, low_s, zero))
        return spot, turn_c, turn_s

    src_spot, src_c, src_s = spot_of(source_row)
    mon_spot, mon_c, mon_s = spot_of(monitor_row)
    scal = jnp.stack(
        [wavenumber, low_c, low_s, high_c, high_s, src_c, src_s, mon_c, -mon_s], axis=1
    )
    spots = jnp.stack([src_spot, mon_spot], axis=1)
    eps_hi, eps_lo = neighbours(*ends(permittivity, 0, REACH))
    eps = jnp.concatenate(
        [permittivity, eps_hi, jnp.ones((TILE - 2 * REACH, width), jnp.float32), eps_lo], axis=0
    )
    hi, lo = neighbours(*ends(warm_field, 2, REACH))
    adj_head, adj_tail = ends(warm_adjoint, 2, REACH)
    adj_head, adj_tail, hi, lo = lax.optimization_barrier((adj_head, adj_tail, hi, lo))
    ahi, alo = neighbours(adj_head, adj_tail)

    smem = pl.BlockSpec(memory_space=pltpu.SMEM)
    field_spec = pl.BlockSpec((1, 2, rows, width), lambda w: (w, 0, 0, 0))
    rim_spec = pl.BlockSpec((1, 2, REACH, width), lambda w: (w, 0, 0, 0))
    row_spec = pl.BlockSpec((1, 2, width), lambda w: (w, 0, 0))
    eps_spec = pl.BlockSpec((total, width), lambda w: (0, 0))
    dot_spec = pl.BlockSpec((1, SUMS, 128), lambda w: (w, 0, 0))
    grad_spec = pl.BlockSpec((rows, width), lambda w: (0, 0))
    field_shape = jax.ShapeDtypeStruct(warm_field.shape, jnp.float32)
    dot_shape = jax.ShapeDtypeStruct((waves, SUMS, 128), jnp.float32)
    ext_shape = pltpu.VMEM((2, total, width), jnp.float32)
    flat_shape = pltpu.VMEM((2, rows, width), jnp.float32)
    params = pltpu.CompilerParams(
        dimension_semantics=("arbitrary",), vmem_limit_bytes=VMEM_LIMIT
    )
    field_bytes = 4 * waves * 2 * rows * width

    def cost(ops, fields):
        return pl.CostEstimate(
            flops=ops * field_bytes // 4, bytes_accessed=fields * field_bytes, transcendentals=0
        )

    dots = pl.pallas_call(
        first_pass,
        grid=(waves,),
        out_shape=dot_shape,
        in_specs=[smem, smem, eps_spec, field_spec, rim_spec, rim_spec, row_spec, row_spec],
        out_specs=dot_spec,
        scratch_shapes=[ext_shape, ext_shape, flat_shape, flat_shape],
        compiler_params=params,
        cost_estimate=cost(60, 1),
        name="first_pass",
    )(scal, spots, eps, warm_field, hi, lo, source_profile, monitor_profile)
    coef = sum_over_gx(dots, True, 0)
    forward, adots = pl.pallas_call(
        second_pass,
        grid=(waves,),
        out_shape=(field_shape, dot_shape),
        in_specs=[smem, smem, smem, eps_spec]
        + [field_spec, rim_spec, rim_spec] * 2
        + [row_spec, row_spec],
        out_specs=(field_spec, dot_spec),
        scratch_shapes=[ext_shape] * 4,
        compiler_params=params,
        cost_estimate=cost(100, 3),
        name="second_pass",
    )(
        scal, spots, coef, eps, warm_field, hi, lo, warm_adjoint, ahi, alo,
        source_profile, monitor_profile,
    )
    acoef = sum_over_gx(adots, False, 1)
    adjoint, grad_part = pl.pallas_call(
        third_pass,
        grid=(waves,),
        out_shape=(field_shape, jax.ShapeDtypeStruct((rows, width), jnp.float32)),
        in_specs=[smem, smem, smem, smem, eps_spec, field_spec, rim_spec, rim_spec, row_spec,
                  field_spec],
        out_specs=(field_spec, grad_spec),
        scratch_shapes=[ext_shape] * 2,
        compiler_params=params,
        cost_estimate=cost(50, 3),
        name="third_pass",
    )(scal, spots, coef, acoef, eps, warm_adjoint, ahi, alo, monitor_profile, forward)
    gradient = gradient_sum(grad_part, design_mask)
    return (forward, adjoint, gradient)


def solution(mesh):
    placed = (
        P("wa", None, "gx", None),
        P("wa", None, "gx", None),
        P("gx", None),
        P("gx", None),
        P("wa"),
        P("wa"),
        P("wa"),
        P("wa"),
        P("wa", None, None),
        P("wa", None, None),
    )
    return jax.shard_map(
        local,
        mesh=mesh,
        in_specs=placed,
        out_specs=(P("wa", None, "gx", None), P("wa", None, "gx", None), P("gx", None)),
        check_vma=False,
    )
```
